32 devices in a mesh: dp: 2 (over x), tp: 4 (over z), ep: 4 (over y, core).
Axes of the slice: x: 2, y: 2, z: 4, core: 2. Of those that a mesh axis runs over, the one named last changes fastest.
Arguments:
- hidden_in: bfloat16 [96, 256, 2048], P(('dp', 'ep'), 'tp'), parts along dimension 0
- ln_attn: float32 [2, 2048], replicated
- ln_ffn: float32 [2, 2048], replicated
- w_query: bfloat16 [2, 2048, 2048], P(None, None, 'tp')
- w_key: bfloat16 [2, 2048, 2048], P(None, None, 'tp')
- w_value: bfloat16 [2, 2048, 2048], P(None, None, 'tp')
- w_out: bfloat16 [2, 2048, 2048], P(None, 'tp')
- bias_table: float32 [2, 16, 32], P(None, 'tp')
- w_gate: bfloat16 [2048, 1024], P(None, 'tp')
- w_up: bfloat16 [2048, 1024], P(None, 'tp')
- w_down: bfloat16 [1024, 2048], P('tp')
- w_router: float32 [2048, 64], replicated
- expert_in: bfloat16 [64, 2048, 1024], P(('tp', 'ep'))
- expert_out: bfloat16 [64, 1024, 2048], P(('tp', 'ep'))
- expert_ids: int32 [96, 256, 2], P(('dp', 'ep'), 'tp'), parts along dimension 0
Outputs:
- output 1: bfloat16 [96, 256, 2048], P(('dp', 'ep'), 'tp'), parts along dimension 0
- output 2: bfloat16 [2, 96, 16, 256, 128], P(None, ('dp', 'ep'), 'tp'), parts along dimension 1
- output 3: bfloat16 [2, 96, 16, 256, 128], P(None, ('dp', 'ep'), 'tp'), parts along dimension 1
There are 2 independent parts. The reference program is written for one: setup_inputs(seed, part) draws one part's arguments, and reference() takes and returns one part's arrays. A program takes and returns all parts, laid end to end along the dimension named above; an argument that names none is the same for every part.
All inputs are finite; a program needn't handle non-finite values.
Results may differ from the reference program's by a relative error of at most 0.0146216.
Values are sent between devices in bfloat16 or wider.
A program may use at most 1 GiB of HBM per device.

```python
import jax
import jax.numpy as jnp
from jax import lax

D_MODEL = 2048
NUM_HEADS = 16
HEAD_DIM = 128
FF_DIM = 1024
NUM_EXPERTS = 64
EP_SIZE = 4
TP_SIZE = 4
BATCH = 48
SEQ_LEN = 256
NUM_BUCKETS = 32
EXACT_BUCKETS = 16

THRESHOLDS = (18, 20, 23, 26, 30, 34, 39, 45, 51, 58, 66, 76, 86, 98, 112)
EPSILON = 1e-6
INNER = NUM_HEADS * HEAD_DIM
LOCAL_BATCH = BATCH // EP_SIZE
LOCAL_SEQ = SEQ_LEN // TP_SIZE
LOCAL_TOKENS = LOCAL_BATCH * LOCAL_SEQ
NUM_GROUPS = EP_SIZE * TP_SIZE
CAPACITY = 4 * LOCAL_TOKENS // NUM_EXPERTS


def draw_ids(id_key):
    coin_key, hot_key, start_key, uniform_key, second_key = jax.random.split(id_key, 5)
    id_shape = (BATCH, SEQ_LEN)
    hot_width = max(NUM_EXPERTS // 8, 1)
    hot_start = jax.random.randint(start_key, (), 0, NUM_EXPERTS)
    hot_pick = (hot_start + jax.random.randint(hot_key, id_shape, 0, hot_width)) % NUM_EXPERTS
    uniform_pick = jax.random.randint(uniform_key, id_shape, 0, NUM_EXPERTS)
    coin_flip = jax.random.randint(coin_key, id_shape, 0, 4)
    first_pick = jnp.where(coin_flip == 0, hot_pick, uniform_pick)
    flat_pos = jnp.arange(BATCH * SEQ_LEN).reshape(id_shape)
    first_pick = jnp.where(flat_pos < NUM_EXPERTS, flat_pos, first_pick)
    second_pick = (first_pick + 1 + jax.random.randint(second_key, id_shape, 0, NUM_EXPERTS - 1)) % NUM_EXPERTS
    return jnp.stack([first_pick, second_pick], axis=-1).astype(jnp.int32)


def setup_inputs(seed: int = 0, part: int = 0) -> dict:
    keys_all = jax.random.split(jax.random.key(seed), 16)
    part_key = jax.random.fold_in(keys_all[0], part)
    act_key, id_key = jax.random.split(part_key)

    def normal(sub_key, dim_tuple, scale_by):
        return jax.random.normal(sub_key, dim_tuple, jnp.float32) * scale_by

    return {
        'hidden_in': normal(act_key, (BATCH, SEQ_LEN, D_MODEL), 1.0).astype(jnp.bfloat16),
        'ln_attn': jax.random.uniform(keys_all[1], (2, D_MODEL), jnp.float32, 0.5, 1.5),
        'ln_ffn': jax.random.uniform(keys_all[2], (2, D_MODEL), jnp.float32, 0.5, 1.5),
        'w_query': normal(keys_all[3], (2, D_MODEL, INNER), D_MODEL ** -0.5).astype(jnp.bfloat16),
        'w_key': normal(keys_all[4], (2, D_MODEL, INNER), D_MODEL ** -0.5).astype(jnp.bfloat16),
        'w_value': normal(keys_all[5], (2, D_MODEL, INNER), D_MODEL ** -0.5).astype(jnp.bfloat16),
        'w_out': normal(keys_all[6], (2, INNER, D_MODEL), INNER ** -0.5).astype(jnp.bfloat16),
        'bias_table': normal(keys_all[7], (2, NUM_HEADS, NUM_BUCKETS), 1.5),
        'w_gate': normal(keys_all[8], (D_MODEL, FF_DIM), D_MODEL ** -0.5).astype(jnp.bfloat16),
        'w_up': normal(keys_all[9], (D_MODEL, FF_DIM), D_MODEL ** -0.5).astype(jnp.bfloat16),
        'w_down': normal(keys_all[10], (FF_DIM, D_MODEL), FF_DIM ** -0.5).astype(jnp.bfloat16),
        'w_router': normal(keys_all[11], (D_MODEL, NUM_EXPERTS), D_MODEL ** -0.5),
        'expert_in': normal(keys_all[12], (NUM_EXPERTS, D_MODEL, FF_DIM), D_MODEL ** -0.5).astype(jnp.bfloat16),
        'expert_out': normal(keys_all[13], (NUM_EXPERTS, FF_DIM, D_MODEL), FF_DIM ** -0.5).astype(jnp.bfloat16),
        'expert_ids': draw_ids(id_key),
    }


def bucket_of(rel_pos):
    bucket_idx = jnp.minimum(rel_pos, EXACT_BUCKETS)
    for threshold in THRESHOLDS:
        bucket_idx = bucket_idx + (rel_pos >= threshold).astype(jnp.int32)
    return bucket_idx


def rms_norm(rows_in, ln_scale):
    wide_rows = rows_in.astype(jnp.float32)
    inv_rms = lax.rsqrt(jnp.mean(wide_rows * wide_rows, axis=-1, keepdims=True) + EPSILON)
    return (wide_rows * inv_rms * ln_scale).astype(jnp.bfloat16)


def causal_bias(bias_rows):
    positions = jnp.arange(SEQ_LEN)
    rel_pos = positions[:, None] - positions[None, :]
    bias_full = jnp.take(bias_rows, bucket_of(jnp.maximum(rel_pos, 0)), axis=1)
    return jnp.where(rel_pos[None] >= 0, bias_full, -jnp.inf)


def attention(hidden, ln_scale, w_query, w_key, w_value, w_out, bias_rows):
    normed = rms_norm(hidden, ln_scale).reshape(BATCH * SEQ_LEN, D_MODEL)

    def project(weight):
        projected = jnp.dot(normed, weight, preferred_element_type=jnp.float32)
        return projected.astype(jnp.bfloat16).reshape(BATCH, SEQ_LEN, NUM_HEADS, HEAD_DIM)

    queries = project(w_query)
    keys_full = project(w_key)
    values_full = project(w_value)
    bias_full = causal_bias(bias_rows)

    def one_sequence(operands):
        query_seq, key_seq, value_seq = operands
        scores = jnp.einsum('qhd,khd->hqk', query_seq.astype(jnp.float32), key_seq.astype(jnp.float32))
        scores = scores * (HEAD_DIM ** -0.5) + bias_full
        attn_probs = jax.nn.softmax(scores, axis=-1).astype(jnp.bfloat16)
        context = jnp.einsum('hqk,khd->qhd', attn_probs.astype(jnp.float32), value_seq.astype(jnp.float32))
        return context.astype(jnp.bfloat16)

    context = lax.map(one_sequence, (queries, keys_full, values_full)).reshape(BATCH * SEQ_LEN, INNER)
    attn_out = jnp.dot(context, w_out, preferred_element_type=jnp.float32).reshape(BATCH, SEQ_LEN, D_MODEL)
    new_hidden = (hidden.astype(jnp.float32) + attn_out).astype(jnp.bfloat16)
    return new_hidden, jnp.swapaxes(keys_full, 1, 2), jnp.swapaxes(values_full, 1, 2)


def dense_ffn(hidden, ln_scale, w_gate, w_up, w_down):
    normed = rms_norm(hidden, ln_scale).reshape(BATCH * SEQ_LEN, D_MODEL)
    gate_pre = jnp.dot(normed, w_gate, preferred_element_type=jnp.float32)
    up_pre = jnp.dot(normed, w_up, preferred_element_type=jnp.float32)
    ffn_hidden = (jax.nn.gelu(gate_pre) * up_pre).astype(jnp.bfloat16)
    ffn_out = jnp.dot(ffn_hidden, w_down, preferred_element_type=jnp.float32).reshape(BATCH, SEQ_LEN, D_MODEL)
    return (hidden.astype(jnp.float32) + ffn_out).astype(jnp.bfloat16)


def to_groups(array_in):
    tail_dims = array_in.shape[2:]
    split_view = array_in.reshape((EP_SIZE, LOCAL_BATCH, TP_SIZE, LOCAL_SEQ) + tail_dims)
    return jnp.swapaxes(split_view, 1, 2).reshape((NUM_GROUPS, LOCAL_TOKENS) + tail_dims)


def from_groups(array_in):
    tail_dims = array_in.shape[2:]
    split_view = array_in.reshape((EP_SIZE, TP_SIZE, LOCAL_BATCH, LOCAL_SEQ) + tail_dims)
    return jnp.swapaxes(split_view, 1, 2).reshape((BATCH, SEQ_LEN) + tail_dims)


def slot_table(choices):
    experts = jnp.arange(NUM_EXPERTS, dtype=jnp.int32)
    first_hot = (choices[..., 0:1] == experts).astype(jnp.int32)
    second_hot = (choices[..., 1:2] == experts).astype(jnp.int32)
    first_pos = jnp.sum((jnp.cumsum(first_hot, axis=-2) - 1) * first_hot, axis=-1)
    second_base = jnp.cumsum(second_hot, axis=-2) - 1 + jnp.sum(first_hot, axis=-2, keepdims=True)
    second_pos = jnp.sum(second_base * second_hot, axis=-1)
    position = jnp.stack([first_pos, second_pos], axis=-1)
    return jnp.where(position < CAPACITY, choices * CAPACITY + position, NUM_EXPERTS * CAPACITY)


def dispatch(group_rows, slot_ids):
    buffer_rows = jnp.zeros((NUM_EXPERTS * CAPACITY + 1, D_MODEL), jnp.bfloat16)
    buffer_rows = buffer_rows.at[slot_ids[:, 0]].set(group_rows).at[slot_ids[:, 1]].set(group_rows)
    return buffer_rows[:-1]


def run_expert(operands):
    rows_in, weight_in, weight_out = operands
    expert_hidden = jax.nn.gelu(jnp.dot(rows_in, weight_in, preferred_element_type=jnp.float32)).astype(jnp.bfloat16)
    return jnp.dot(expert_hidden, weight_out, preferred_element_type=jnp.float32).astype(jnp.bfloat16)


def gather_rows(table_rows, slot_ids):
    return jnp.take(table_rows, slot_ids, axis=0)


def moe_layer(hidden, ln_scale, w_router, expert_in, expert_out, expert_ids):
    tok_rows = to_groups(rms_norm(hidden, ln_scale))
    choices = to_groups(expert_ids)
    logits = jnp.einsum('gnd,de->gne', tok_rows.astype(jnp.float32), w_router)
    router_probs = jax.nn.softmax(logits, axis=-1)
    picked = jnp.take_along_axis(router_probs, choices, axis=-1)
    gate_weights = picked / jnp.sum(picked, axis=-1, keepdims=True)
    slot_ids = slot_table(choices)
    buffers = jax.vmap(dispatch)(tok_rows, slot_ids)
    per_expert = jnp.swapaxes(buffers.reshape(NUM_GROUPS, NUM_EXPERTS, CAPACITY, D_MODEL), 0, 1)
    per_expert = per_expert.reshape(NUM_EXPERTS, NUM_GROUPS * CAPACITY, D_MODEL)
    expert_result = lax.map(run_expert, (per_expert, expert_in, expert_out))
    returned = jnp.swapaxes(expert_result.reshape(NUM_EXPERTS, NUM_GROUPS, CAPACITY, D_MODEL), 0, 1)
    returned = returned.reshape(NUM_GROUPS, NUM_EXPERTS * CAPACITY, D_MODEL)
    padded = jnp.concatenate([returned, jnp.zeros((NUM_GROUPS, 1, D_MODEL), jnp.bfloat16)], axis=1)
    gathered_out = jax.vmap(gather_rows)(padded, slot_ids)
    moe_sum = jnp.sum(gate_weights[..., None] * gathered_out.astype(jnp.float32), axis=2)
    return (hidden.astype(jnp.float32) + from_groups(moe_sum)).astype(jnp.bfloat16)


def reference(hidden_in, ln_attn, ln_ffn, w_query, w_key, w_value, w_out, bias_table, w_gate, w_up, w_down, w_router, expert_in, expert_out, expert_ids):
    hidden, keys_zero, values_zero = attention(hidden_in, ln_attn[0], w_query[0], w_key[0], w_value[0], w_out[0], bias_table[0])
    hidden = dense_ffn(hidden, ln_ffn[0], w_gate, w_up, w_down)
    hidden, keys_one, values_one = attention(hidden, ln_attn[1], w_query[1], w_key[1], w_value[1], w_out[1], bias_table[1])
    hidden = moe_layer(hidden, ln_ffn[1], w_router, expert_in, expert_out, expert_ids)
    return hidden, jnp.stack([keys_zero, keys_one]), jnp.stack([values_zero, values_one])
```

```python
import jax
import jax.numpy as jnp
from jax import lax
from jax.sharding import PartitionSpec as P

EXACT_BUCKETS = 16
THRESHOLDS = (18, 20, 23, 26, 30, 34, 39, 45, 51, 58, 66, 76, 86, 98, 112)
EPSILON = 1e-6


def bucket_of(rel_pos):
    bucket_idx = jnp.minimum(rel_pos, EXACT_BUCKETS)
    for threshold in THRESHOLDS:
        bucket_idx = bucket_idx + (rel_pos >= threshold).astype(jnp.int32)
    return bucket_idx


def rms_norm(rows_in, ln_scale):
    wide_rows = rows_in.astype(jnp.float32)
    inv_rms = lax.rsqrt(jnp.mean(wide_rows * wide_rows, axis=-1, keepdims=True) + EPSILON)
    return (wide_rows * inv_rms * ln_scale).astype(jnp.bfloat16)


def causal_bias(bias_rows, seq_len):
    positions = jnp.arange(seq_len)
    rel_pos = (positions[:, None] - positions[None, :])[None]
    starts = tuple(range(EXACT_BUCKETS + 1)) + THRESHOLDS
    bias_full = jnp.broadcast_to(bias_rows[:, 0][:, None, None], (bias_rows.shape[0], seq_len, seq_len))
    for bucket, start in enumerate(starts[1:], 1):
        bias_full = jnp.where(rel_pos >= start, bias_rows[:, bucket][:, None, None], bias_full)
    return jnp.where(rel_pos >= 0, bias_full, -jnp.inf)


def attend(normed_full, w_query, w_key, w_value, bias_full):
    local_batch, seq_len, d_model = normed_full.shape
    num_heads = bias_full.shape[0]
    head_dim = w_query.shape[1] // num_heads

    def project(weight):
        projected = jnp.einsum('btd,dk->btk', normed_full, weight, preferred_element_type=jnp.float32)
        return projected.astype(jnp.bfloat16).reshape(local_batch, seq_len, num_heads, head_dim)

    queries = project(w_query)
    keys_full = project(w_key)
    values_full = project(w_value)
    scores = jnp.einsum('bqhd,bkhd->bhqk', queries, keys_full, preferred_element_type=jnp.float32)
    scores = scores * (head_dim ** -0.5) + bias_full[None]
    attn_probs = jax.nn.softmax(scores, axis=-1).astype(jnp.bfloat16)
    context = jnp.einsum('bhqk,bkhd->bqhd', attn_probs, values_full, preferred_element_type=jnp.float32)
    context = context.astype(jnp.bfloat16).reshape(local_batch, seq_len, num_heads * head_dim)
    return context, jnp.swapaxes(keys_full, 1, 2), jnp.swapaxes(values_full, 1, 2)


def after(values, anchor):
    return lax.optimization_barrier((values, anchor))


def gather_weight(piece):
    return lax.all_gather(piece, ('tp', 'dp', 'ep'), axis=0, tiled=True)


def shard_piece(local, parts, index):
    rows = local.shape[0] // parts
    return lax.dynamic_slice_in_dim(local, index * rows, rows, axis=0)


def add_rows(hidden, lhs, weight):
    product = jnp.einsum('btf,fd->btd', lhs, weight, preferred_element_type=jnp.float32)
    return (hidden.astype(jnp.float32) + product).astype(jnp.bfloat16)


def ffn_rows(hidden, ln_scale, w_gate, w_up, w_down):
    normed = rms_norm(hidden, ln_scale)
    gate_pre = jnp.einsum('btd,fd->btf', normed, w_gate, preferred_element_type=jnp.float32)
    up_pre = jnp.einsum('btd,fd->btf', normed, w_up, preferred_element_type=jnp.float32)
    ffn_hidden = (jax.nn.gelu(gate_pre) * up_pre).astype(jnp.bfloat16)
    return add_rows(hidden, ffn_hidden, w_down)


def slot_table(choices, num_experts):
    experts = jnp.arange(num_experts, dtype=jnp.int32)
    first_hot = (choices[..., 0:1] == experts).astype(jnp.int32)
    second_hot = (choices[..., 1:2] == experts).astype(jnp.int32)
    first_pos = jnp.sum((jnp.cumsum(first_hot, axis=-2) - 1) * first_hot, axis=-1)
    second_base = jnp.cumsum(second_hot, axis=-2) - 1 + jnp.sum(first_hot, axis=-2, keepdims=True)
    second_pos = jnp.sum(second_base * second_hot, axis=-1)
    return jnp.stack([first_pos, second_pos], axis=-1)


def moe_plan(choices, num_experts, capacity):
    experts = jnp.arange(num_experts, dtype=jnp.int32)
    position = slot_table(choices, num_experts)
    hot = choices[:, :, None] == experts
    slot_ids = jnp.where(position < capacity, choices * capacity + position, -1)
    return slot_ids, hot


def moe_block(hidden, ln_scale, w_router, expert_in, expert_out, plan):
    slot_ids, hot = plan
    local_batch, local_seq, d_model = hidden.shape
    tokens = local_batch * local_seq
    num_experts = w_router.shape[1]
    local_experts = expert_in.shape[0]
    groups = num_experts // local_experts
    capacity = 4 * tokens // num_experts
    axes = ('tp', 'ep')
    normed = rms_norm(hidden, ln_scale).reshape(tokens, d_model)
    wide = normed.astype(jnp.float32)
    slot_order = jnp.arange(num_experts * capacity, dtype=jnp.int32).reshape(groups, local_experts, capacity)
    logits = jnp.dot(wide, w_router, precision=lax.Precision.HIGHEST)
    router_probs = jax.nn.softmax(logits, axis=-1)
    picked = jnp.sum(jnp.where(hot, router_probs[:, None, :], 0.0), axis=-1)
    gate_weights = picked / jnp.sum(picked, axis=-1, keepdims=True)

    returned = []
    step = local_experts // PARTS
    for part in range(PARTS):
        columns = slot_order[:, part * step:(part + 1) * step].reshape(-1)
        select = ((slot_ids[:, 0, None] == columns) | (slot_ids[:, 1, None] == columns)).astype(jnp.bfloat16)
        rows_out = jnp.einsum('ns,nd->sd', select, normed, preferred_element_type=jnp.float32).astype(jnp.bfloat16)
        received = lax.all_to_all(rows_out, axes, 0, 0, tiled=True).reshape(groups, step, capacity, d_model)
        results = []
        for item in range(step):
            expert = part * step + item
            expert_hidden = jnp.einsum('gcd,df->gcf', received[:, item], expert_in[expert], preferred_element_type=jnp.float32)
            expert_hidden = jax.nn.gelu(expert_hidden).astype(jnp.bfloat16)
            result = jnp.einsum('gcf,fd->gcd', expert_hidden, expert_out[expert], preferred_element_type=jnp.float32)
            results.append(result.astype(jnp.bfloat16))
        result = jnp.stack(results, axis=1).reshape(groups * step * capacity, d_model)
        returned.append(lax.all_to_all(result, axes, 0, 0, tiled=True))
    moe_sum = None
    for part in range(PARTS):
        columns = slot_order[:, part * step:(part + 1) * step].reshape(-1)
        rows_back = returned[part]
        if part:
            rows_back, moe_sum = after(rows_back, moe_sum)
        one_hot = (slot_ids[:, :, None] == columns).astype(jnp.bfloat16)
        chosen = jnp.einsum('ncs,sd->ncd', one_hot, rows_back, preferred_element_type=jnp.float32)
        part_sum = jnp.sum(gate_weights[:, :, None] * chosen, axis=1)
        moe_sum = part_sum if moe_sum is None else moe_sum + part_sum
    moe_sum = moe_sum.reshape(local_batch, local_seq, d_model)
    return (hidden.astype(jnp.float32) + moe_sum).astype(jnp.bfloat16)


CHUNKS = 2
PARTS = 2


def solution(mesh):
    act_spec = P(('dp', 'ep'), 'tp', None)
    col_spec = P(None, None, 'tp')
    row_spec = P(None, 'tp', None)
    expert_spec = P(('tp', 'ep'), None, None)
    cache_spec = P(None, ('dp', 'ep'), 'tp', None, None)
    in_specs = (act_spec, P(), P(), col_spec, col_spec, col_spec, row_spec, row_spec,
                P(None, 'tp'), P(None, 'tp'), P('tp', None), P(), expert_spec, expert_spec, act_spec)
    tp_size = mesh.shape['tp']
    plane = mesh.shape['dp'] * mesh.shape['ep']

    def device_fn(hidden_in, ln_attn, ln_ffn, w_query, w_key, w_value, w_out, bias_table, w_gate, w_up, w_down, w_router, expert_in, expert_out, expert_ids):
        local_batch, local_seq, d_model = hidden_in.shape
        seq_len = local_seq * tp_size
        spot = lax.axis_index(('dp', 'ep'))
        size = local_batch // CHUNKS
        tokens = local_batch * local_seq
        num_experts = w_router.shape[1]
        plan = moe_plan(expert_ids.reshape(tokens, 2), num_experts, 4 * tokens // num_experts)

        parts_zero = [shard_piece(w_out[0], plane, spot), shard_piece(w_gate.T, plane, spot),
                      shard_piece(w_up.T, plane, spot), shard_piece(w_down, plane, spot)]
        piece_zero = jnp.concatenate(parts_zero, axis=0)
        piece_one = shard_piece(w_out[1], plane, spot)
        biases = [causal_bias(bias_table[layer], seq_len) for layer in range(2)]

        def gather(rows):
            return lax.all_gather(rows, 'tp', axis=1, tiled=True)

        keys, values = [[], []], [[], []]

        def attention(layer, gathered):
            context, keys_new, values_new = attend(gathered, w_query[layer], w_key[layer], w_value[layer], biases[layer])
            keys[layer].append(keys_new)
            values[layer].append(values_new)
            context = context.reshape(size, tp_size, local_seq, context.shape[-1])
            return jnp.swapaxes(context, 0, 1)

        def project_out(rows, context, weight):
            weight = weight.reshape(tp_size, -1, d_model)
            product = jnp.einsum('sbtf,sfd->btd', context, weight, preferred_element_type=jnp.float32)
            return (rows.astype(jnp.float32) + product).astype(jnp.bfloat16)

        def attention_chain(layer, gathered):
            arrived, own = [], None
            for rows in gathered:
                if own is not None:
                    rows, own = after(rows, own)
                    arrived.append(lax.all_to_all(own, 'tp', 0, 0, tiled=True))
                own = attention(layer, rows)
                if arrived:
                    own, arrived[-1] = after(own, arrived[-1])
            arrived.append(lax.all_to_all(own, 'tp', 0, 0, tiled=True))
            return arrived

        hidden = [hidden_in[c * size:(c + 1) * size] for c in range(CHUNKS)]
        gathered = [gather(rms_norm(rows, ln_attn[0])) for rows in hidden]
        piece_zero, gathered[-1] = after(piece_zero, gathered[-1])
        joined = gather_weight(piece_zero).reshape(tp_size * plane, -1, d_model)
        weights_zero, first = [], 0
        for part in parts_zero:
            weights_zero.append(joined[:, first:first + part.shape[0]].reshape(-1, d_model))
            first += part.shape[0]
        out_zero, gate, up, down = weights_zero
        contexts = attention_chain(0, gathered)
        gathered = []
        for c in range(CHUNKS):
            rows = hidden[c]
            if c:
                rows, normed = after(rows, normed)
                gathered.append(gather(normed))
            rows = project_out(rows, contexts[c], out_zero)
            rows = ffn_rows(rows, ln_ffn[0], gate, up, down)
            hidden[c] = rows
            normed = rms_norm(rows, ln_attn[1])
        gathered.append(gather(normed))
        piece_one, gathered[0] = after(piece_one, gathered[0])
        out_one = gather_weight(piece_one)
        contexts = attention_chain(1, gathered)
        hidden = jnp.concatenate([project_out(hidden[c], contexts[c], out_one) for c in range(CHUNKS)], axis=0)
        hidden = moe_block(hidden, ln_ffn[1], w_router, expert_in, expert_out, plan)

        def cache(parts):
            return jnp.stack([jnp.concatenate(rows, axis=0) for rows in parts])

        return hidden, cache(keys), cache(values)

    return jax.shard_map(device_fn, mesh=mesh, in_specs=in_specs, out_specs=(act_spec, cache_spec, cache_spec), check_vma=False)
```

```python
import jax
import jax.numpy as jnp
from jax import lax
from jax.sharding import PartitionSpec as P

EXACT_BUCKETS = 16
THRESHOLDS = (18, 20, 23, 26, 30, 34, 39, 45, 51, 58, 66, 76, 86, 98, 112)
EPSILON = 1e-6


def bucket_of(rel_pos):
    bucket_idx = jnp.minimum(rel_pos, EXACT_BUCKETS)
    for threshold in THRESHOLDS:
        bucket_idx = bucket_idx + (rel_pos >= threshold).astype(jnp.int32)
    return bucket_idx


def rms_norm(rows_in, ln_scale):
    wide_rows = rows_in.astype(jnp.float32)
    inv_rms = lax.rsqrt(jnp.mean(wide_rows * wide_rows, axis=-1, keepdims=True) + EPSILON)
    return (wide_rows * inv_rms * ln_scale).astype(jnp.bfloat16)


def causal_bias(bias_rows, seq_len):
    positions = jnp.arange(seq_len)
    rel_pos = (positions[:, None] - positions[None, :])[None]
    starts = tuple(range(EXACT_BUCKETS + 1)) + THRESHOLDS
    bias_full = jnp.broadcast_to(bias_rows[:, 0][:, None, None], (bias_rows.shape[0], seq_len, seq_len))
    for bucket, start in enumerate(starts[1:], 1):
        bias_full = jnp.where(rel_pos >= start, bias_rows[:, bucket][:, None, None], bias_full)
    return jnp.where(rel_pos >= 0, bias_full, -jnp.inf)


def attend(normed_full, w_query, w_key, w_value, bias_full):
    local_batch, seq_len, d_model = normed_full.shape
    num_heads = bias_full.shape[0]
    head_dim = w_query.shape[1] // num_heads

    def project(weight):
        projected = jnp.einsum('btd,dk->btk', normed_full, weight, preferred_element_type=jnp.float32)
        return projected.astype(jnp.bfloat16).reshape(local_batch, seq_len, num_heads, head_dim)

    queries = project(w_query)
    keys_full = project(w_key)
    values_full = project(w_value)
    scores = jnp.einsum('bqhd,bkhd->bhqk', queries, keys_full, preferred_element_type=jnp.float32)
    scores = scores * (head_dim ** -0.5) + bias_full[None]
    attn_probs = jax.nn.softmax(scores, axis=-1).astype(jnp.bfloat16)
    context = jnp.einsum('bhqk,bkhd->bqhd', attn_probs, values_full, preferred_element_type=jnp.float32)
    context = context.astype(jnp.bfloat16).reshape(local_batch, seq_len, num_heads * head_dim)
    return context, jnp.swapaxes(keys_full, 1, 2), jnp.swapaxes(values_full, 1, 2)


def after(values, anchor):
    return lax.optimization_barrier((values, anchor))


def swap_pairs(blocks, axis, pairs):
    return blocks + [lax.ppermute(block, axis, pairs) for block in blocks]


def shard_piece(local, parts, index):
    rows = local.shape[0] // parts
    return lax.dynamic_slice_in_dim(local, index * rows, rows, axis=0)


def add_rows(hidden, lhs, weight):
    product = jnp.einsum('btf,fd->btd', lhs, weight, preferred_element_type=jnp.float32)
    return (hidden.astype(jnp.float32) + product).astype(jnp.bfloat16)


def ffn_rows(hidden, ln_scale, w_gate, w_up, w_down):
    normed = rms_norm(hidden, ln_scale)
    gate_pre = jnp.einsum('btd,fd->btf', normed, w_gate, preferred_element_type=jnp.float32)
    up_pre = jnp.einsum('btd,fd->btf', normed, w_up, preferred_element_type=jnp.float32)
    ffn_hidden = (jax.nn.gelu(gate_pre) * up_pre).astype(jnp.bfloat16)
    return add_rows(hidden, ffn_hidden, w_down)


def slot_table(choices, num_experts):
    experts = jnp.arange(num_experts, dtype=jnp.int32)
    first_hot = (choices[..., 0:1] == experts).astype(jnp.int32)
    second_hot = (choices[..., 1:2] == experts).astype(jnp.int32)
    first_pos = jnp.sum((jnp.cumsum(first_hot, axis=-2) - 1) * first_hot, axis=-1)
    second_base = jnp.cumsum(second_hot, axis=-2) - 1 + jnp.sum(first_hot, axis=-2, keepdims=True)
    second_pos = jnp.sum(second_base * second_hot, axis=-1)
    return jnp.stack([first_pos, second_pos], axis=-1)


def moe_plan(choices, num_experts, capacity):
    experts = jnp.arange(num_experts, dtype=jnp.int32)
    position = slot_table(choices, num_experts)
    hot = choices[:, :, None] == experts
    slot_ids = jnp.where(position < capacity, choices * capacity + position, -1)
    return slot_ids, hot


def moe_block(hidden, ln_scale, w_router, expert_in, expert_out, plan):
    slot_ids, hot = plan
    local_batch, local_seq, d_model = hidden.shape
    tokens = local_batch * local_seq
    num_experts = w_router.shape[1]
    local_experts = expert_in.shape[0]
    groups = num_experts // local_experts
    capacity = 4 * tokens // num_experts
    axes = ('tp', 'ep')
    normed = rms_norm(hidden, ln_scale).reshape(tokens, d_model)
    wide = normed.astype(jnp.float32)
    slot_order = jnp.arange(num_experts * capacity, dtype=jnp.int32).reshape(groups, local_experts, capacity)
    logits = jnp.dot(wide, w_router, precision=lax.Precision.HIGHEST)
    router_probs = jax.nn.softmax(logits, axis=-1)
    picked = jnp.sum(jnp.where(hot, router_probs[:, None, :], 0.0), axis=-1)
    gate_weights = picked / jnp.sum(picked, axis=-1, keepdims=True)

    returned = []
    step = local_experts // PARTS
    for part in range(PARTS):
        columns = slot_order[:, part * step:(part + 1) * step].reshape(-1)
        select = ((slot_ids[:, 0, None] == columns) | (slot_ids[:, 1, None] == columns)).astype(jnp.bfloat16)
        rows_out = jnp.einsum('ns,nd->sd', select, normed, preferred_element_type=jnp.float32).astype(jnp.bfloat16)
        received = lax.all_to_all(rows_out, axes, 0, 0, tiled=True).reshape(groups, step, capacity, d_model)
        results = []
        for item in range(step):
            expert = part * step + item
            expert_hidden = jnp.einsum('gcd,df->gcf', received[:, item], expert_in[expert], preferred_element_type=jnp.float32)
            expert_hidden = jax.nn.gelu(expert_hidden).astype(jnp.bfloat16)
            result = jnp.einsum('gcf,fd->gcd', expert_hidden, expert_out[expert], preferred_element_type=jnp.float32)
            results.append(result.astype(jnp.bfloat16))
        result = jnp.stack(results, axis=1).reshape(groups * step * capacity, d_model)
        returned.append(lax.all_to_all(result, axes, 0, 0, tiled=True))
    moe_sum = None
    for part in range(PARTS):
        columns = slot_order[:, part * step:(part + 1) * step].reshape(-1)
        rows_back = returned[part]
        if part:
            rows_back, moe_sum = after(rows_back, moe_sum)
        one_hot = (slot_ids[:, :, None] == columns).astype(jnp.bfloat16)
        chosen = jnp.einsum('ncs,sd->ncd', one_hot, rows_back, preferred_element_type=jnp.float32)
        part_sum = jnp.sum(gate_weights[:, :, None] * chosen, axis=1)
        moe_sum = part_sum if moe_sum is None else moe_sum + part_sum
    moe_sum = moe_sum.reshape(local_batch, local_seq, d_model)
    return (hidden.astype(jnp.float32) + moe_sum).astype(jnp.bfloat16)


CHUNKS = 2
PARTS = 2


def solution(mesh):
    act_spec = P(('dp', 'ep'), 'tp', None)
    col_spec = P(None, None, 'tp')
    row_spec = P(None, 'tp', None)
    expert_spec = P(('tp', 'ep'), None, None)
    cache_spec = P(None, ('dp', 'ep'), 'tp', None, None)
    in_specs = (act_spec, P(), P(), col_spec, col_spec, col_spec, row_spec, row_spec,
                P(None, 'tp'), P(None, 'tp'), P('tp', None), P(), expert_spec, expert_spec, act_spec)
    tp_size = mesh.shape['tp']
    dp_size, ep_size = mesh.shape['dp'], mesh.shape['ep']
    plane = dp_size * ep_size

    def device_fn(hidden_in, ln_attn, ln_ffn, w_query, w_key, w_value, w_out, bias_table, w_gate, w_up, w_down, w_router, expert_in, expert_out, expert_ids):
        local_batch, local_seq, d_model = hidden_in.shape
        seq_len = local_seq * tp_size
        spot = lax.axis_index(('dp', 'ep'))
        size = local_batch // CHUNKS
        tokens = local_batch * local_seq
        num_experts = w_router.shape[1]
        plan = moe_plan(expert_ids.reshape(tokens, 2), num_experts, 4 * tokens // num_experts)

        parts_zero = [shard_piece(w_out[0], plane, spot), shard_piece(w_gate.T, plane, spot),
                      shard_piece(w_up.T, plane, spot), shard_piece(w_down, plane, spot),
                      shard_piece(w_out[1], plane, spot)]
        piece_zero = jnp.concatenate(parts_zero, axis=0)
        biases = [causal_bias(bias_table[layer], seq_len) for layer in range(2)]

        def gather(rows):
            return lax.all_gather(rows, 'tp', axis=1, tiled=True)

        keys, values = [[], []], [[], []]

        def attention(layer, gathered):
            context, keys_new, values_new = attend(gathered, w_query[layer], w_key[layer], w_value[layer], biases[layer])
            keys[layer].append(keys_new)
            values[layer].append(values_new)
            context = context.reshape(size, tp_size, local_seq, context.shape[-1])
            return jnp.swapaxes(context, 0, 1)

        def project_out(rows, context, weight):
            weight = weight.reshape(tp_size, -1, d_model)
            product = jnp.einsum('sbtf,sfd->btd', context, weight, preferred_element_type=jnp.float32)
            return (rows.astype(jnp.float32) + product).astype(jnp.bfloat16)

        def swap_heads(context):
            return lax.all_to_all(context, 'tp', 0, 0, tiled=True)

        def attention_zero(gathered):
            context = jnp.concatenate([attention(0, rows) for rows in gathered], axis=1)
            arrived = swap_heads(context)
            return [arrived[:, c * size:(c + 1) * size] for c in range(CHUNKS)]

        def attention_one(gathered):
            arrived, own = [], None
            for rows in gathered:
                if own is not None:
                    arrived.append(swap_heads(own))
                    rows, arrived[-1] = after(rows, arrived[-1])
                own = attention(1, rows)
            arrived.append(swap_heads(own))
            return arrived

        hidden = [hidden_in[c * size:(c + 1) * size] for c in range(CHUNKS)]
        normed = [rms_norm(rows, ln_attn[0]) for rows in hidden]
        column = lax.all_gather(piece_zero, 'tp', axis=0)
        normed, column = after(normed, column)
        gathered = [gather(rows) for rows in normed]
        blocks = swap_pairs([column], 'dp', [(i, i ^ 1) for i in range(dp_size)])
        for bit in (2, 1):
            blocks = swap_pairs(blocks, 'ep', [(i, i ^ bit) for i in range(ep_size)])
        order = [(r & 1) * ep_size + (r & 2) + (r >> 2) for r in range(plane)]
        blocks = [blocks[order.index(q)] for q in range(plane)]
        weights_zero, first = [], 0
        for number, part in enumerate(parts_zero):
            last = first + part.shape[0]
            whole = jnp.stack([block[:, first:last] for block in blocks])
            if number in (0, 4):
                ranks = [lax.dynamic_index_in_dim(whole, spot ^ q, 0, keepdims=False) for q in range(plane)]
                whole = jnp.stack(ranks, axis=1)
            weights_zero.append(whole.reshape(-1, d_model))
            first = last
        out_zero, gate, up, down, out_one = weights_zero
        contexts = attention_zero(gathered)
        gathered = []
        for c in range(CHUNKS):
            rows = hidden[c]
            if c:
                gathered.append(gather(normed))
                rows, _ = after(rows, normed)
            rows = project_out(rows, contexts[c], out_zero)
            rows = ffn_rows(rows, ln_ffn[0], gate, up, down)
            hidden[c] = rows
            normed = rms_norm(rows, ln_attn[1])
        gathered.append(gather(normed))
        contexts = attention_one(gathered)
        hidden = jnp.concatenate([project_out(hidden[c], contexts[c], out_one) for c in range(CHUNKS)], axis=0)
        hidden = moe_block(hidden, ln_ffn[1], w_router, expert_in, expert_out, plan)

        def cache(parts):
            return jnp.stack([jnp.concatenate(rows, axis=0) for rows in parts])

        return hidden, cache(keys), cache(values)

    return jax.shard_map(device_fn, mesh=mesh, in_specs=in_specs, out_specs=(act_spec, cache_spec, cache_spec), check_vma=False)
```
